32 devices in a mesh: rows: 8 (over y, x, core), cols: 4 (over z).
Axes of the slice: x: 2, y: 2, z: 4, core: 2. Of those that a mesh axis runs over, the one named last changes fastest.
Arguments:
- memory: float32 [128, 262144], P('cols', 'rows'), may hold values from -3 to 3
- last_tick: int32 [262144], P('rows'), may hold values from 0 to 999
- slot_node: int32 [64, 256], P('rows'), may hold values from 0 to 262143, as said below
- slot_pair: int32 [64, 256], P('rows'), may hold values from 0 to 2047, as said below
- slot_tick: int32 [64, 256], P('rows'), may hold values from 1000 to 1999
- block_count: int32 [8, 8], P('rows'), may hold values from 0 to 256, as said below
- time_freq: float32 [128], replicated, may hold values from 0.002 to 0.1
- time_phase: float32 [128], replicated, may hold values from -3.140625 to 3.140625
- w_pair: bfloat16 [128, 2, 384], P('cols'), may hold values from -0.3125 to 0.3125
- w_time: bfloat16 [128, 384], P('cols'), may hold values from -0.3125 to 0.3125
- w_hidden: bfloat16 [128, 384], P('cols'), may hold values from -0.5 to 0.5
- bias_input: float32 [384], P('cols'), may hold values from -3 to 3
- bias_hidden: float32 [384], P('cols'), may hold values from -3 to 3
Outputs:
- new_memory: float32 [128, 262144], P('cols', 'rows')
The draws below stay inside these ranges and needn't reach their ends.
Inputs may be any that keep to these rules, and one draw needn't show every extreme that they name: `slot_node`: every slot of block b (live or not) names a node of owner b, from b * 32768 to (b + 1) * 32768 - 1. `slot_pair`: indexes the holder's 8 * 256 slots flattened block by block; the relation is symmetric without fixed points, and live slots pair with live slots. `block_count`: every count is even; in every draw one owner's block is full (256 live slots) from every holder.
All inputs are finite; a program needn't handle non-finite values.
Results may differ from the reference program's by a relative error of at most 0.0006.
Values may be sent and summed in bfloat16 or wider, within the bound.
A program may use at most 128 MiB of HBM per device.

```python
import math
import jax
import jax.numpy as jnp
from jax import lax

MEM = 128
TDIM = 128
NODE_DEV = 32768
CAP = 256
TICK_SPAN = 1000
NODES = 262144
N_ROWS = 8


def layout_all(key):
    base_key = jax.random.fold_in(key, 7)
    hot_key, count_key, node_key, order_key = jax.random.split(base_key, 4)
    hottest = jax.random.randint(hot_key, (), 0, N_ROWS)
    drawn = 2 * jax.random.randint(count_key, (N_ROWS, N_ROWS), CAP // 16, 5 * CAP // 32 + 1)
    counts = jnp.where(jnp.arange(N_ROWS)[None, :] == hottest, CAP, drawn).astype(jnp.int32)
    local = jax.random.randint(node_key, (N_ROWS, N_ROWS, CAP), 0, NODE_DEV)
    nodes = (jnp.arange(N_ROWS)[None, :, None] * NODE_DEV + local).astype(jnp.int32)
    span = N_ROWS * CAP
    filled = (jnp.arange(CAP)[None, None, :] < counts[:, :, None]).reshape(N_ROWS, span)
    ranks = jax.vmap(lambda k: jax.random.permutation(k, span))(jax.random.split(order_key, N_ROWS))
    score = jnp.where(filled, 0, span) + ranks
    order = jnp.argsort(score, axis=1, stable=True).astype(jnp.int32)
    flipped = jnp.arange(span) ^ 1

    def pair_row(row_order):
        return jnp.zeros((span,), jnp.int32).at[row_order].set(row_order[flipped])
    pairs = jax.vmap(pair_row)(order)
    return (counts, nodes.reshape(N_ROWS * N_ROWS, CAP), pairs.reshape(N_ROWS * N_ROWS, CAP))


def draw_block_count(key, part):
    return layout_all(key)[0]


def draw_slot_node(key, part):
    return layout_all(key)[1]


def draw_slot_pair(key, part):
    return layout_all(key)[2]


def set_ends(values, stream_key, low, high):
    longest = values.shape.index(max(values.shape))
    spots = []
    for shift in (0, 1):
        where = [jax.random.randint(jax.random.fold_in(stream_key, axis), (), 0, length) for axis, length in enumerate(values.shape)]
        where[longest] = (where[longest] + shift) % values.shape[longest]
        spots.append(tuple(where))
    return values.at[spots[0]].set(low).at[spots[1]].set(high)


def block_scale(rng, shape, pieces, low, largest):
    loudness = 1.0
    for position, shards_of in pieces:
        heights = jax.random.uniform(jax.random.fold_in(jax.random.fold_in(rng, 6), position), (shards_of,), jnp.float32, low / len(pieces), largest / len(pieces))
        loudness = loudness * jnp.repeat(jnp.exp(heights), shape[position] // shards_of).reshape((-1,) + (1,) * (len(shape) - 1 - position))
    return loudness


def centred(key, shape, scale, most, cuts=(), kind=jnp.bfloat16):
    level = block_scale(key, shape, cuts, -0.22, 0.18) if cuts else 1.0
    drawn = jax.random.normal(key, shape, jnp.float32) * scale * level
    return jnp.minimum(jnp.maximum(drawn, -most), most).astype(kind)


def setup_inputs(seed: int = 0) -> dict:
    keys = jax.random.split(jax.random.key(seed), 14)
    return {
        "memory": centred(keys[0], (MEM, NODES), 0.5, 3.0, ((0, 4), (1, 8)), jnp.float32),
        "last_tick": set_ends(jax.random.randint(keys[1], (NODES,), 0, TICK_SPAN), jax.random.fold_in(keys[1], 1), 0, TICK_SPAN - 1).astype(jnp.int32),
        "slot_node": draw_slot_node(jax.random.fold_in(keys[13], 71), 0),
        "slot_pair": draw_slot_pair(jax.random.fold_in(keys[13], 71), 0),
        "slot_tick": set_ends(jax.random.randint(keys[4], (N_ROWS * N_ROWS, CAP), TICK_SPAN, 2 * TICK_SPAN), jax.random.fold_in(keys[4], 1), TICK_SPAN, (2 * TICK_SPAN) - 1).astype(jnp.int32),
        "block_count": draw_block_count(jax.random.fold_in(keys[13], 71), 0),
        "time_freq": jnp.clip(jnp.exp(jax.random.uniform(keys[6], (TDIM,), jnp.float32, math.log(0.002), math.log(0.1))), 0.002, 0.1),
        "time_phase": jnp.clip(jax.random.uniform(keys[7], (TDIM,), jnp.float32, -3.140625, 3.140625), -3.140625, 3.140625),
        "w_pair": centred(keys[8], (MEM, 2, 3 * MEM), (2 * MEM + TDIM) ** -0.5, 0.3125, ((0, 4),)),
        "w_time": centred(keys[9], (TDIM, 3 * MEM), (2 * MEM + TDIM) ** -0.5, 0.3125, ((0, 4),)),
        "w_hidden": centred(keys[10], (MEM, 3 * MEM), MEM ** -0.5, 0.5, ((0, 4),)),
        "bias_input": centred(keys[11], (3 * MEM,), 0.5, 3.0, ((0, 4),), jnp.float32),
        "bias_hidden": centred(keys[12], (3 * MEM,), 0.5, 3.0, ((0, 4),), jnp.float32),
    }


def reference(memory, last_tick, slot_node, slot_pair, slot_tick, block_count, time_freq, time_phase, w_pair, w_time, w_hidden, bias_input, bias_hidden):
    width = memory.shape[0]
    slots = slot_node.reshape(N_ROWS, N_ROWS, CAP)
    flat_nodes = slot_node.reshape(N_ROWS, N_ROWS * CAP)
    partners = jnp.take_along_axis(flat_nodes, slot_pair.reshape(N_ROWS, N_ROWS * CAP), axis=1).reshape(N_ROWS, N_ROWS, CAP)
    ticks = slot_tick.reshape(N_ROWS, N_ROWS, CAP)
    filled = jnp.arange(CAP, dtype=jnp.int32)[None, None, :] < block_count[:, :, None]

    def owner_block(owner):
        nodes = slots[:, owner].reshape(-1)
        others = partners[:, owner].reshape(-1)
        live = filled[:, owner].reshape(-1)
        hidden = memory[:, nodes].T
        self_in = hidden.astype(jnp.bfloat16)
        partner_in = memory[:, others].T.astype(jnp.bfloat16)
        gaps = (ticks[:, owner].reshape(-1) - last_tick[nodes]).astype(jnp.float32)
        encoded = jnp.cos(gaps[:, None] * time_freq[None, :] + time_phase[None, :]).astype(jnp.bfloat16)
        gate_in = jnp.dot(self_in, w_pair[:, 0, :], preferred_element_type=jnp.float32)
        gate_in = gate_in + jnp.dot(partner_in, w_pair[:, 1, :], preferred_element_type=jnp.float32)
        gate_in = gate_in + jnp.dot(encoded, w_time, preferred_element_type=jnp.float32)
        gate_hid = jnp.dot(self_in, w_hidden, preferred_element_type=jnp.float32)
        local = jnp.where(live, nodes - owner * NODE_DEV, NODE_DEV).astype(jnp.int32)
        sums = jnp.zeros((NODE_DEV + 1, 3 * width), jnp.float32).at[local].add(gate_in)
        counts = jnp.zeros((NODE_DEV + 1,), jnp.float32).at[NODE_DEV].set(1.0).at[local].add(1.0)
        mean = sums[local] / counts[local][:, None]
        gx = (mean + bias_input[None, :]).reshape(-1, width, 3)
        gh = (gate_hid + bias_hidden[None, :]).reshape(-1, width, 3)
        reset = jax.nn.sigmoid(gx[:, :, 0] + gh[:, :, 0])
        keep = jax.nn.sigmoid(gx[:, :, 1] + gh[:, :, 1])
        cand = jnp.tanh(gx[:, :, 2] + reset * gh[:, :, 2])
        fresh = (1.0 - keep) * cand + keep * hidden
        block = lax.dynamic_slice_in_dim(memory, owner * NODE_DEV, NODE_DEV, 1)
        return block.at[:, local].set(fresh.T, mode="drop")

    result = lax.map(owner_block, jnp.arange(N_ROWS, dtype=jnp.int32))
    return jnp.transpose(result, (1, 0, 2)).reshape(width, N_ROWS * NODE_DEV)
```

```python
import functools

import jax
import jax.numpy as jnp
from jax import lax
from jax.experimental import pallas as pl
from jax.experimental.pallas import tpu as pltpu
from jax.sharding import PartitionSpec as P

MESH = pl.DeviceIdType.MESH
LANES = 128
SHIFT = 16
VM = pl.BlockSpec(memory_space=pltpu.VMEM)
SM = pl.BlockSpec(memory_space=pltpu.SMEM)
ANY = pl.BlockSpec(memory_space=pl.ANY)
PIECES = 8
F32, I32, B16 = jnp.float32, jnp.int32, jnp.bfloat16


def mate(me, k, n, back=False):
    if n & (n - 1):
        return lax.rem(me + (n - k if back else k), n)
    out = me
    for i in range(n.bit_length() - 1):
        if k >> i & 1:
            out = out + (1 << i) * (1 - 2 * lax.rem(lax.div(me, 1 << i), 2))
    return out


def remote(src, dst, send, recv, axis, peer):
    return pltpu.make_async_remote_copy(
        src_ref=src,
        dst_ref=dst,
        send_sem=send,
        recv_sem=recv,
        device_id={axis: peer},
        device_id_type=MESH,
    )


def chain(c, block, first, places, sems):
    col = lax.axis_index("cols")
    n = len(places)
    ways = (True, False)

    def hop(source, t, k, right):
        send, recv = sems[0:2] if right else sems[2:4]
        ref = block(source, places[k])
        return remote(
            first(k) if t == 0 else ref,
            ref,
            send.at[t, k],
            recv.at[t, k],
            "cols",
            col + 1 if right else col - 1,
        )

    def goes(right):
        return col < c - 1 if right else col > 0

    def where_from(t, right):
        source = col - t if right else col + t
        there = source >= 0 if right else source < c
        return source, there

    def begin(k):
        for right in ways:

            @pl.when(goes(right))
            def _(right=right):
                hop(col, 0, k, right).start()

    def rest(done):
        for t in range(1, c):
            for k in range(n):
                for right in ways:
                    source, there = where_from(t, right)

                    @pl.when(there)
                    def _(right=right, source=source, t=t, k=k):
                        hop(source, t - 1, k, right).wait_recv()

                    @pl.when(jnp.logical_and(there, goes(right)))
                    def _(right=right, source=source, t=t, k=k):
                        hop(source, t, k, right).start()

                if t == c - 1:
                    done(k)

        for t in range(c - 1):
            for right in ways:
                source, there = where_from(t, right)

                @pl.when(jnp.logical_and(there, goes(right)))
                def _(right=right, source=source, t=t):
                    for k in range(n):
                        hop(source, t, k, right).wait_send()

    return begin, rest


def lanes_of(i, width):
    return pl.ds(pl.multiple_of(i * width, width), width)


def spread_row(ref, hit):
    return jnp.sum(jnp.where(hit, ref[...], 0.0), axis=1, keepdims=True)


def over_in(a, b):
    return lax.dot_general(a, b, (((0,), (0,)), ((), ())), preferred_element_type=F32)


def iota(shape, axis):
    return lax.broadcasted_iota(I32, shape, axis)


def main_kernel(
    n,
    c,
    nodes,
    ticks,
    counts,
    pair,
    last,
    w_pair,
    w_time,
    w_hid,
    bias_in,
    bias_hid,
    freq,
    phase,
    memory,
    meta,
    fresh,
    rows_out,
    flat,
    rows,
    ids,
    meta_src,
    w_src,
    w,
    picked,
    own,
    held,
    wide,
    where,
    perm,
    self_all,
    part_all,
    gaps,
    columns,
    equal,
    inverse,
    timed,
    pre,
    acc,
    load_sem,
    save_sem,
    id_sem,
    meta_s,
    meta_r,
    w_s,
    w_r,
    reply_s,
    reply_r,
    self_s,
    self_r,
    spread_s,
    spread_r,
    *hops,
):
    row, col = lax.axis_index("rows"), lax.axis_index("cols")
    cap = nodes.shape[1]
    wp, node_rows = memory.shape
    groups = LANES // wp
    rows_n = node_rows // groups
    g3 = 3 * wp
    per = cap // LANES
    tiles = n * per
    width = c * g3

    barrier = pltpu.get_barrier_semaphore()
    for axis, size, me in (("rows", n, row), ("cols", c, col)):
        for k in range(1, size):
            pl.semaphore_signal(
                barrier, inc=1, device_id={axis: mate(me, k, size)}, device_id_type=MESH
            )

    step = rows_n // PIECES
    loads = []
    for i in range(PIECES):
        for k in range(groups):
            part = pl.ds(k * rows_n + i * step, step)
            loads.append(pltpu.make_async_copy(memory.at[:, part], flat.at[:, part], load_sem.at[i, k]))
    for copy in loads:
        copy.start()

    lane = iota((1, cap), 1)
    for b in range(n):
        mine = nodes[b : b + 1, :] - b * node_rows
        group = jnp.zeros((1, cap), I32)
        for k in range(1, groups):
            group = group + jnp.where(mine >= k * rows_n, 1, 0)
        code = mine + group * ((1 << SHIFT) - rows_n)
        meta_src[b, 0:1, :] = jnp.where(lane < counts[0, b], code, rows_n)
        meta_src[b, 1:2, :] = ticks[b : b + 1, :]

    pl.semaphore_wait(barrier, n + c - 2)
    metas = [
        remote(
            meta_src.at[mate(row, k, n)],
            meta.at[row],
            meta_s.at[k],
            meta_r.at[k],
            "rows",
            mate(row, k, n),
        )
        for k in range(1, n)
    ]
    for copy in reversed(metas):
        copy.start()
    meta[row] = meta_src[row]

    q = iota((1, LANES), 1)
    gate = jnp.zeros((1, LANES), I32)
    for k in range(1, 4):
        gate = gate + jnp.where(q >= k * wp, 1, 0)
    target = jnp.where(q < g3, 3 * (q - gate * wp) + gate, -width)
    stacked = jnp.concatenate([w_pair[:, 0, :], w_pair[:, 1, :], w_time[...], w_hid[...]], axis=0)
    from_col = iota((width, LANES), 0)
    for p in range(c):
        pick = jnp.where(from_col == target + p * g3, 1.0, 0.0).astype(B16)
        block = jnp.dot(stacked, pick, preferred_element_type=F32).astype(B16)
        for k in range(4):
            w_src[p, k] = block[k * wp : (k + 1) * wp]
    sends = [
        remote(
            w_src.at[mate(col, k, c)], w.at[col], w_s.at[k], w_r.at[k], "cols", mate(col, k, c)
        )
        for k in range(1, c)
    ]
    for copy in sends:
        copy.start()
    w[col] = w_src[col]

    rows[rows_n:, :] = jnp.zeros((8, LANES), F32)
    per_piece = step // LANES

    def turn(i, _):
        block = [flat[:, lanes_of(k * (rows_n // LANES) + i, LANES)] for k in range(groups)]
        rows[lanes_of(i, LANES), :] = jnp.concatenate(block, 0).T
        return 0

    saves = []
    for i in range(PIECES):
        for k in range(groups):
            loads[i * groups + k].wait()
        lax.fori_loop(i * per_piece, (i + 1) * per_piece, turn, 0, unroll=8)
        part = pl.ds(i * step, step)
        saves.append(pltpu.make_async_copy(rows.at[part], rows_out.at[part], save_sem.at[i]))
        saves[-1].start()

    sources = [mate(row, k, n, True) for k in range(n)]
    others = [mate(row, k, n) for k in range(n)]
    id_copies = [
        pltpu.make_async_copy(meta.at[sources[k]], ids.at[sources[k]], id_sem.at[k])
        for k in range(n)
    ]

    def arrive(k):
        if k:
            remote(
                meta_src.at[others[k]],
                meta.at[sources[k]],
                meta_s.at[k],
                meta_r.at[k],
                "rows",
                others[k],
            ).wait_recv()
        id_copies[k].start()

    def reply(k):
        b = sources[k]
        return remote(
            self_all.at[col, b], held.at[row], reply_s.at[k], reply_r.at[k], "rows", b
        )

    def reply_in(k):
        return remote(
            self_all.at[col, others[k]],
            held.at[others[k]],
            reply_s.at[k],
            reply_r.at[k],
            "rows",
            others[k],
        )

    def self_out(k, j):
        ref = self_all.at[col, sources[k]]
        return remote(ref, ref, self_s.at[j, k], self_r.at[j, k], "cols", mate(col, j, c))

    def self_in(k, j):
        ref = self_all.at[mate(col, j, c, True), sources[k]]
        return remote(ref, ref, self_s.at[j, k], self_r.at[j, k], "cols", mate(col, j, c))

    def gather(b):
        def slot(j, _):
            for u in range(32):
                r = lax.bitwise_and(ids[b, 0, j * 32 + u], (1 << SHIFT) - 1)
                picked[pl.ds(j * 32 + u, 1), :] = rows[pl.ds(r, 1), :]
            return 0

        lax.fori_loop(0, cap // 32, slot, 0)
        for half in range(per):
            lanes = slice(half * LANES, (half + 1) * LANES)
            group = lax.shift_right_logical(meta[b, 0:1, lanes], SHIFT)
            turned = picked[lanes, :].T
            mine = turned[0:wp]
            for k in range(1, groups):
                mine = jnp.where(group == k, turned[k * wp : (k + 1) * wp], mine)
            own[:, lanes_of(b * per + half, LANES)] = mine
            self_all[col, b, :, lanes] = mine.astype(B16)

    arrive(0)
    for k in range(n):
        if k + 1 < n:
            arrive(k + 1)
        id_copies[k].wait()
        gather(sources[k])
        if k:
            reply(k).start()
        else:
            held[row] = self_all[col, row]
        for j in reversed(range(1, c)):
            self_out(k, j).start()

    low, high = [], []
    hi_rows = node_rows // LANES
    old = last[...]
    table = jnp.concatenate(
        [lax.shift_right_logical(old, 8).astype(F32), lax.bitwise_and(old, 255).astype(F32)], axis=1
    ).astype(B16)
    hi_iota = iota((hi_rows, cap), 0)
    lo_iota = iota((LANES, cap), 0)

    def gap_of(b, _):
        code = meta[b, 0:1, :]
        r = lax.bitwise_and(code, (1 << SHIFT) - 1)
        hi = lax.shift_right_logical(r, 7) + lax.shift_right_logical(code, SHIFT) * (rows_n // LANES)
        pick = jnp.where(hi_iota == hi, 1.0, 0.0).astype(B16)
        found = over_in(table, pick)
        found = found[0:LANES] * 256.0 + found[LANES:]
        found = jnp.where(lo_iota == lax.bitwise_and(r, LANES - 1), found, 0.0)
        gaps[b] = meta[b, 1:2, :].astype(F32) - jnp.sum(found, axis=0, keepdims=True)
        return 0

    lax.fori_loop(0, n, gap_of, 0)

    for k in range(tiles):
        half = slice((k % per) * LANES, (k % per + 1) * LANES)
        where[k : k + 1, :] = pair[k // per : k // per + 1, half]

    def column(i, _):
        block, half = lax.div(i, per), lax.rem(i, per)
        code = meta[block, 0:1, lanes_of(half, LANES)].astype(F32)
        columns[lanes_of(i, LANES), :] = jnp.broadcast_to(code, (LANES, LANES)).T
        return 0

    lax.fori_loop(0, tiles, column, 0, unroll=4)

    for k in range(1, n):
        reply_in(k).wait_recv()

    for k in range(tiles):
        wide[k] = held[k // per, :, (k % per) * LANES : (k % per + 1) * LANES].astype(F32)

    def permute(block, _):
        for half in range(per):
            p = where[pl.ds(block * per + half, 1), :]
            tile = jnp.broadcast_to(lax.shift_right_logical(p, 7), (8, LANES))
            place = jnp.broadcast_to(lax.bitwise_and(p, LANES - 1), (8, LANES))
            parts = [jnp.zeros((8, LANES), F32) for _ in range(wp // 8)]
            for k in range(tiles):
                hit = tile == k
                for r in range(wp // 8):
                    got = jnp.take_along_axis(wide[k, r * 8 : (r + 1) * 8, :], place, axis=1)
                    parts[r] = jnp.where(hit, got, parts[r])
            whole = jnp.concatenate(parts, axis=0).astype(B16)
            perm[block, :, half * LANES : (half + 1) * LANES] = whole
        return 0

    lax.fori_loop(0, n, permute, 0)

    spreads = [
        remote(
            perm.at[others[k]],
            part_all.at[col, row],
            spread_s.at[k],
            spread_r.at[k],
            "rows",
            others[k],
        )
        for k in range(1, n)
    ]
    for copy in spreads:
        copy.start()

    def spread_in(k):
        return remote(
            perm.at[others[k]],
            part_all.at[col, sources[k]],
            spread_s.at[k],
            spread_r.at[k],
            "rows",
            others[k],
        )

    begin, rest = chain(
        c,
        lambda source, place: part_all.at[source, place],
        lambda k: part_all.at[col, sources[k]] if k else perm.at[row],
        sources,
        hops,
    )
    begin(0)
    part_all[col, row] = perm[row]

    def same_of(i, _):
        block, half = lax.div(i, per), lax.rem(i, per)
        code = meta[block, 0:1, lanes_of(half, LANES)].astype(F32)
        same = jnp.where(columns[...] == code, 1.0, 0.0)
        equal[:, lanes_of(i, LANES)] = same.astype(B16)
        inverse[:, lanes_of(i, LANES)] = 1.0 / jnp.sum(same, axis=0, keepdims=True)
        return 0

    lax.fori_loop(0, tiles, same_of, 0)
    for k in range(1, n):
        spread_in(k).wait_recv()
        begin(k)

    for k in range(1, c):
        remote(
            w_src.at[mate(col, k, c)],
            w.at[mate(col, k, c, True)],
            w_s.at[k],
            w_r.at[k],
            "cols",
            mate(col, k, c),
        ).wait_recv()
    w_self, w_part, w_time_all, w_hid_all = (
        w[:, k].reshape(c * wp, LANES)[:, 0:g3] for k in range(4)
    )
    to_row = iota((g3, g3), 0)
    to_gate = jnp.zeros((g3, g3), I32)
    for k in range(1, 3):
        to_gate = to_gate + jnp.where(to_row >= k * wp, 1, 0)
    hit = iota((g3, g3), 1) == 3 * (to_row - to_gate * wp) + to_gate
    bias_x, bias_h = spread_row(bias_in, hit), spread_row(bias_hid, hit)
    square = (freq.shape[1],) * 2
    diagonal = iota(square, 0) == iota(square, 1)
    rate, shift_by = spread_row(freq, diagonal), spread_row(phase, diagonal)
    acc[...] = jnp.zeros(acc.shape, F32)

    def time_part(b, _):
        encoded = jnp.cos(gaps[b] * rate + shift_by).astype(B16)
        timed[:, lanes_of(b, cap)] = over_in(w_time_all, encoded)
        return 0

    lax.fori_loop(0, n, time_part, 0)

    for k in range(n):
        for j in range(1, c):
            self_in(k, j).wait_recv()

    def self_part(b, _):
        lanes = lanes_of(b, cap)
        xs = self_all[:, b].reshape(c * wp, cap)
        gx = over_in(w_self, xs) + bias_x
        gh = over_in(w_hid_all, xs) + bias_h
        pre[0 : 2 * wp, lanes] = gx[0 : 2 * wp] + gh[0 : 2 * wp]
        pre[2 * wp : 3 * wp, lanes] = gx[2 * wp :]
        pre[3 * wp :, lanes] = gh[2 * wp :]
        return 0

    lax.fori_loop(0, n, self_part, 0)

    def add_block(k):
        b = sources[k]
        xp = part_all[:, b].reshape(c * wp, cap)
        gi = over_in(w_part, xp) + timed[:, lanes_of(b, cap)]
        big = gi.astype(B16)
        both = jnp.concatenate([big, (gi - big.astype(F32)).astype(B16)], axis=0)
        mine = pl.ds(pl.multiple_of(b * cap, cap), cap)

        def into(i, _):
            lanes = lanes_of(i, cap)
            sums = jnp.dot(both, equal[mine, lanes], preferred_element_type=F32)
            acc[:, lanes] += sums[0:g3] + sums[g3:]
            return 0

        lax.fori_loop(0, n, into, 0)

    rest(add_block)

    def gates(b, _):
        lanes = lanes_of(b, cap)
        mean = acc[:, lanes] * inverse[:, lanes]
        rz = jax.nn.sigmoid(mean[0 : 2 * wp] + pre[0 : 2 * wp, lanes])
        reset, keep = rz[0:wp], rz[wp:]
        cand = jnp.tanh(mean[2 * wp :] + pre[2 * wp : 3 * wp, lanes] + reset * pre[3 * wp :, lanes])
        fresh[:, lanes] = (1.0 - keep) * cand + keep * own[:, lanes]
        return 0

    lax.fori_loop(0, n, gates, 0)

    for copy in saves:
        copy.wait()
    for copy in metas + sends + spreads:
        copy.wait_send()
    for k in range(n):
        if k:
            reply(k).wait_send()
        for j in range(1, c):
            self_out(k, j).wait_send()


def scatter_kernel(ids, fresh, rows_in, out, flat, rows, turned, load_sem, out_sem):
    n, _, cap = ids.shape
    wp, node_rows = out.shape
    groups = LANES // wp
    rows_n = node_rows // groups
    tiles = n * cap // LANES
    step = rows_n // PIECES
    loads = [
        pltpu.make_async_copy(
            rows_in.at[pl.ds(i * step, step)], rows.at[pl.ds(i * step, step)], load_sem.at[i]
        )
        for i in range(PIECES)
    ]
    for copy in loads:
        copy.start()

    def tile(i, _):
        value = fresh[:, lanes_of(i, LANES)]
        turned[lanes_of(i, LANES), :] = jnp.concatenate([value] * groups, axis=0).T
        return 0

    lax.fori_loop(0, tiles, tile, 0, unroll=4)
    for copy in loads:
        copy.wait()
    group_of = lax.div(iota((1, LANES), 1), wp)

    def slots(b, _):
        def slot(j, _):
            for u in range(32):
                code = ids[b, 0, j * 32 + u]
                r = lax.bitwise_and(code, (1 << SHIFT) - 1)
                pltpu.store(
                    rows.at[pl.ds(r, 1), :],
                    turned[pl.ds(b * cap + j * 32 + u, 1), :],
                    mask=group_of == lax.shift_right_logical(code, SHIFT),
                )
            return 0

        lax.fori_loop(0, cap // 32, slot, 0)
        return 0

    lax.fori_loop(0, n, slots, 0)
    per_piece = step // LANES

    def back(i, _):
        x = rows[lanes_of(i, LANES), :].T
        for k in range(groups):
            flat[:, lanes_of(k * (rows_n // LANES) + i, LANES)] = x[k * wp : (k + 1) * wp]
        return 0

    copies = []
    for i in range(PIECES):
        lax.fori_loop(i * per_piece, (i + 1) * per_piece, back, 0, unroll=8)
        for k in range(groups):
            part = pl.ds(k * rows_n + i * step, step)
            copies.append(pltpu.make_async_copy(flat.at[:, part], out.at[:, part], out_sem.at[i, k]))
            copies[-1].start()
    for copy in copies:
        copy.wait()


def dma(*shape):
    return pltpu.SemaphoreType.DMA(shape)


def local(
    n,
    c,
    memory,
    last_tick,
    slot_node,
    slot_pair,
    slot_tick,
    block_count,
    time_freq,
    time_phase,
    w_pair,
    w_time,
    w_hidden,
    bias_input,
    bias_hidden,
):
    wp, node_rows = memory.shape
    cap = slot_node.shape[1]
    total = n * cap
    tiles = total // LANES
    g3 = 3 * wp
    groups = LANES // wp
    rows_n = node_rows // groups
    shape = jax.ShapeDtypeStruct
    vm = pltpu.VMEM
    meta, fresh, rows = pl.pallas_call(
        functools.partial(main_kernel, n, c),
        out_shape=(
            shape((n, 2, cap), I32),
            shape((wp, total), F32),
            shape((rows_n, LANES), F32),
        ),
        in_specs=[VM, VM, SM] + [VM] * 9 + [ANY],
        out_specs=(VM, VM, ANY),
        scratch_shapes=[
            vm((wp, node_rows), F32),
            vm((rows_n + 8, LANES), F32),
            pltpu.SMEM((n, 2, cap), I32),
            vm((n, 2, cap), I32),
            vm((c, 4, wp, LANES), B16),
            vm((c, 4, wp, LANES), B16),
            vm((cap, LANES), F32),
            vm((wp, total), F32),
            vm((n, wp, cap), B16),
            vm((tiles, wp, LANES), F32),
            vm((tiles, LANES), I32),
            vm((n, wp, cap), B16),
            vm((c, n, wp, cap), B16),
            vm((c, n, wp, cap), B16),
            vm((n, 1, cap), F32),
            vm((total, LANES), F32),
            vm((total, total), B16),
            vm((1, total), F32),
            vm((g3, total), F32),
            vm((4 * wp, total), F32),
            vm((g3, total), F32),
            dma(PIECES, groups),
            dma(PIECES),
            dma(n),
            dma(n),
            dma(n),
            dma(c),
            dma(c),
            dma(n),
            dma(n),
            dma(c, n),
            dma(c, n),
            dma(n),
            dma(n),
        ]
        + [dma(c, n)] * 4,
        compiler_params=pltpu.CompilerParams(collective_id=1, has_side_effects=True),
        name="exchange",
    )(
        slot_node,
        slot_tick,
        block_count,
        slot_pair,
        last_tick.reshape(node_rows // LANES, LANES),
        w_pair,
        w_time,
        w_hidden,
        bias_input.reshape(1, g3),
        bias_hidden.reshape(1, g3),
        time_freq.reshape(1, -1),
        time_phase.reshape(1, -1),
        memory,
    )
    return pl.pallas_call(
        scatter_kernel,
        out_shape=shape((wp, node_rows), F32),
        in_specs=[SM, VM, ANY],
        out_specs=ANY,
        scratch_shapes=[
            vm((wp, node_rows), F32),
            vm((rows_n + 8, LANES), F32),
            vm((total, LANES), F32),
            dma(PIECES),
            dma(PIECES, groups),
        ],
        name="scatter",
    )(meta, fresh, rows)


def solution(mesh):
    placed = (
        P("cols", "rows"),
        P("rows"),
        P("rows", None),
        P("rows", None),
        P("rows", None),
        P("rows", None),
        P(),
        P(),
        P("cols", None, None),
        P("cols", None),
        P("cols", None),
        P("cols"),
        P("cols"),
    )
    return jax.shard_map(
        functools.partial(local, mesh.shape["rows"], mesh.shape["cols"]),
        mesh=mesh,
        in_specs=placed,
        out_specs=P("cols", "rows"),
        check_vma=False,
    )
```

```python
import functools

import jax
import jax.numpy as jnp
from jax import lax
from jax.experimental import pallas as pl
from jax.experimental.pallas import tpu as pltpu
from jax.sharding import PartitionSpec as P

MESH = pl.DeviceIdType.MESH
LANES = 128
SHIFT = 16
VM = pl.BlockSpec(memory_space=pltpu.VMEM)
SM = pl.BlockSpec(memory_space=pltpu.SMEM)
ANY = pl.BlockSpec(memory_space=pl.ANY)
HBM = pl.BlockSpec(memory_space=pltpu.HBM)
PIECES = 4
VMEM_BYTES = 67_043_328
SELF_PARTS = 2
F32, I32, B16 = jnp.float32, jnp.int32, jnp.bfloat16


def mate(me, k, n, back=False):
    if n & (n - 1):
        return lax.rem(me + (n - k if back else k), n)
    out = me
    for i in range(n.bit_length() - 1):
        if k >> i & 1:
            out = out + (1 << i) * (1 - 2 * lax.rem(lax.div(me, 1 << i), 2))
    return out


def remote(src, dst, send, recv, axis, peer):
    return pltpu.make_async_remote_copy(
        src_ref=src,
        dst_ref=dst,
        send_sem=send,
        recv_sem=recv,
        device_id={axis: peer},
        device_id_type=MESH,
    )


def ladder(c, buffer, first, places, parts, sends, recvs):
    col = lax.axis_index("cols")
    ways = (True, False)
    n = len(places)
    each = n // parts

    def towards(steps, right):
        return col + steps if right else col - steps

    def has(d, right):
        return towards(-d, right) >= 0 if right else towards(-d, right) < c

    def fits(d, right):
        return towards(d, right) < c if right else towards(d, right) >= 0

    def send_sem(d, right):
        return sends.at[2 * d + right]

    def hop(d, k, right, stride):
        source = towards(stride - d, right)
        ref = buffer.at[source, places[k]]
        return remote(
            first(k) if d == stride else ref,
            ref,
            send_sem(d, right),
            recvs.at[source, k // each],
            "cols",
            towards(stride, right),
        )

    def landed(d, part, right):
        source = towards(-d, right)
        peer = jnp.minimum(col + 1, c - 1) if right else jnp.maximum(col - 1, 0)
        ref = buffer.at[source, pl.ds(0, each)]
        return remote(ref, ref, send_sem(d, right), recvs.at[source, part], "cols", peer)

    def when(*tests):
        return pl.when(functools.reduce(jnp.logical_and, tests))

    def begin(k):
        for d in (2, 1):
            for right in ways:
                if d < c:

                    @when(fits(d, right))
                    def _(d=d, right=right):
                        hop(d, k, right, d).start()

    def forward(part):
        for d in range(2, c - 1):
            for right in ways:

                @when(has(d, right), fits(1, right))
                def _(d=d, right=right):
                    landed(d, part, right).wait_recv()
                    for k in range(part * each, (part + 1) * each):
                        hop(d + 1, k, right, 1).start()

    def finish(part):
        for d in range(1, c):
            for right in ways:
                tests = [has(d, right)]
                if d > 1:
                    tests.append(jnp.logical_not(fits(1, right)))

                @when(*tests)
                def _(d=d, right=right):
                    landed(d, part, right).wait_recv()

    def drain():
        for right in ways:
            peer = jnp.minimum(col + 1, c - 1) if right else jnp.maximum(col - 1, 0)
            for d in range(1, c):
                if d < 3:
                    tests = [fits(d, right)]
                else:
                    tests = [has(d - 1, right), fits(1, right)]

                @when(*tests)
                def _(d=d, right=right, peer=peer):
                    ref = buffer.at[0]
                    remote(ref, ref, send_sem(d, right), recvs.at[0, 0], "cols", peer).wait_send()

    return begin, forward, finish, drain


def lanes_of(i, width):
    return pl.ds(pl.multiple_of(i * width, width), width)


def spread_row(ref, hit):
    return jnp.sum(jnp.where(hit, ref[...], 0.0), axis=1, keepdims=True)


def over_in(a, b):
    return lax.dot_general(a, b, (((0,), (0,)), ((), ())), preferred_element_type=F32)


def iota(shape, axis):
    return lax.broadcasted_iota(I32, shape, axis)


def main_kernel(n, c, *refs):
    given, memory, refs = refs[0:12], refs[12], refs[13:]
    meta, fresh, rows, refs = *refs[0:3], refs[3:]
    taken, in_sem, refs = refs[0:12], refs[12], refs[13:]
    fetches = [
        pltpu.make_async_copy(a, b, in_sem.at[i]) for i, (a, b) in enumerate(zip(given, taken))
    ]
    main_body(n, c, fetches, *taken, memory, meta, fresh, rows, *refs)


def main_body(
    n,
    c,
    fetches,
    nodes,
    ticks,
    counts,
    pair,
    last,
    w_pair,
    w_time,
    w_hid,
    bias_in,
    bias_hid,
    freq,
    phase,
    memory,
    meta,
    fresh,
    rows,
    flat,
    ids,
    meta_src,
    w_src,
    w,
    picked,
    own,
    held,
    wide,
    where,
    perm,
    self_all,
    part_all,
    gaps,
    columns,
    equal,
    number,
    timed,
    pre,
    acc,
    load_sem,
    id_sem,
    meta_s,
    meta_r,
    w_s,
    w_r,
    reply_s,
    reply_r,
    spread_s,
    spread_r,
    *hops,
):
    row, col = lax.axis_index("rows"), lax.axis_index("cols")
    cap = nodes.shape[1]
    wp, node_rows = memory.shape
    groups = LANES // wp
    rows_n = node_rows // groups
    g3 = 3 * wp
    per = cap // LANES
    tiles = n * per
    width = c * g3

    def group_row(b, half):
        return lax.shift_right_logical(meta[b, pl.ds(per + half, 1), :], SHIFT)

    def node_row(b, half):
        return meta[b, pl.ds(half, 1), :] + group_row(b, half) * rows_n

    def wide_row(row_of, b):
        return jnp.concatenate([row_of(b, half) for half in range(per)], axis=1)

    barrier = pltpu.get_barrier_semaphore()
    for axis, size, me in (("rows", n, row), ("cols", c, col)):
        for k in range(1, size):
            pl.semaphore_signal(
                barrier, inc=1, device_id={axis: mate(me, k, size)}, device_id_type=MESH
            )

    for copy in fetches:
        copy.start()
    step = rows_n // PIECES
    loads = []
    for i in range(PIECES):
        for k in range(groups):
            part = pl.ds(k * rows_n + i * step, step)
            loads.append(pltpu.make_async_copy(memory.at[:, part], flat.at[:, part], load_sem.at[i]))
    for copy in loads:
        copy.start()

    lane = iota((1, cap), 1)
    for copy in fetches[0:3]:
        copy.wait()
    for b in range(n):
        mine = nodes[b : b + 1, :] - b * node_rows
        group = jnp.zeros((1, cap), I32)
        for k in range(1, groups):
            group = group + jnp.where(mine >= k * rows_n, 1, 0)
        live = lane < counts[0:1, b : b + 1]
        place = jnp.where(live, mine - group * rows_n, rows_n)
        rest_of = ticks[b : b + 1, :] + jnp.where(live, group, groups) * (1 << SHIFT)
        for half in range(per):
            lanes = slice(half * LANES, (half + 1) * LANES)
            meta_src[b, half : half + 1, :] = place[:, lanes]
            meta_src[b, per + half : per + half + 1, :] = rest_of[:, lanes]

    pl.semaphore_wait(barrier, n + c - 2)
    metas = [
        remote(
            meta_src.at[mate(row, k, n)],
            meta.at[row],
            meta_s.at[0],
            meta_r.at[k],
            "rows",
            mate(row, k, n),
        )
        for k in range(1, n)
    ]
    for copy in reversed(metas):
        copy.start()
    meta[row] = meta_src[row]

    for copy in fetches[3:]:
        copy.wait()
    q = iota((1, LANES), 1)
    gate = jnp.zeros((1, LANES), I32)
    for k in range(1, 4):
        gate = gate + jnp.where(q >= k * wp, 1, 0)
    target = jnp.where(q < g3, 3 * (q - gate * wp) + gate, -width)
    stacked = jnp.concatenate([w_pair[:, 0, :], w_pair[:, 1, :], w_time[...], w_hid[...]], axis=0)
    from_col = iota((width, LANES), 0)
    for p in range(c):
        pick = jnp.where(from_col == target + p * g3, 1.0, 0.0).astype(B16)
        block = jnp.dot(stacked, pick, preferred_element_type=F32).astype(B16)
        for k in range(4):
            w_src[p, k] = block[k * wp : (k + 1) * wp]
    sends = [
        remote(
            w_src.at[mate(col, k, c)], w.at[col], w_s.at[0], w_r.at[0], "cols", mate(col, k, c)
        )
        for k in range(1, c)
    ]
    for copy in sends:
        copy.start()
    w[col] = w_src[col]

    rows[rows_n:, :] = jnp.zeros((8, LANES), F32)
    per_piece = step // LANES

    def turn(i, _):
        block = [flat[:, lanes_of(k * (rows_n // LANES) + i, LANES)] for k in range(groups)]
        rows[lanes_of(i, LANES), :] = jnp.concatenate(block, 0).T
        return 0

    for i in range(PIECES):
        all_groups = pl.ds(0, groups * step)
        pltpu.make_async_copy(
            memory.at[:, all_groups], flat.at[:, all_groups], load_sem.at[i]
        ).wait()
        lax.fori_loop(i * per_piece, (i + 1) * per_piece, turn, 0, unroll=8)

    sources = [mate(row, k, n, True) for k in range(n)]
    others = [mate(row, k, n) for k in range(n)]
    id_copies = [
        pltpu.make_async_copy(meta.at[sources[k]], ids.at[sources[k]], id_sem.at[k])
        for k in range(n)
    ]

    def arrive(k):
        if k:
            remote(
                meta_src.at[others[k]],
                meta.at[sources[k]],
                meta_s.at[0],
                meta_r.at[k],
                "rows",
                others[k],
            ).wait_recv()
        id_copies[k].start()

    def reply(k):
        b = sources[k]
        return remote(
            self_all.at[col, b], held.at[row], reply_s.at[0], reply_r.at[0], "rows", b
        )

    rest = pl.ds(0, n - 1)
    reply_in = remote(
        self_all.at[col, rest], held.at[rest], reply_s.at[0], reply_r.at[0], "rows", others[1]
    )

    begin_self, forward_self, finish_self, drain_self = ladder(
        c, self_all, lambda k: self_all.at[col, sources[k]], sources, SELF_PARTS, *hops[0:2]
    )
    begin, forward, finish, drain = ladder(
        c,
        part_all,
        lambda k: part_all.at[col, sources[k]] if k else perm.at[row],
        sources,
        n,
        *hops[2:4],
    )

    def gather(b):
        def slots(half, _):
            for u in range(LANES):
                picked[pl.ds(half * LANES + u, 1), :] = rows[pl.ds(ids[b, half, u], 1), :]
            return 0

        lax.fori_loop(0, per, slots, 0)
        for half in range(per):
            lanes = slice(half * LANES, (half + 1) * LANES)
            group = group_row(b, half)
            turned = picked[lanes, :].T
            mine = turned[0:wp]
            for k in range(1, groups):
                mine = jnp.where(group == k, turned[k * wp : (k + 1) * wp], mine)
            own[:, lanes_of(b * per + half, LANES)] = mine
            self_all[col, b, :, lanes] = mine.astype(B16)

    arrive(0)
    for k in range(n):
        if k + 1 < n:
            arrive(k + 1)
        id_copies[k].wait()
        gather(sources[k])
        if k:
            reply(k).start()
        else:
            held[row] = self_all[col, row]
        begin_self(k)

    hi_rows = node_rows // LANES
    old = last[...]
    table = jnp.concatenate(
        [lax.shift_right_logical(old, 8).astype(F32), lax.bitwise_and(old, 255).astype(F32)], axis=1
    ).astype(B16)
    hi_iota = iota((hi_rows, cap), 0)
    lo_iota = iota((LANES, cap), 0)

    def gap_of(b, _):
        node = wide_row(node_row, b)
        pick = jnp.where(hi_iota == lax.shift_right_logical(node, 7), 1.0, 0.0).astype(B16)
        found = over_in(table, pick)
        found = found[0:LANES] * 256.0 + found[LANES:]
        found = jnp.where(lo_iota == lax.bitwise_and(node, LANES - 1), found, 0.0)
        tick = wide_row(lambda b, half: meta[b, pl.ds(per + half, 1), :], b)
        tick = lax.bitwise_and(tick, (1 << SHIFT) - 1).astype(F32)
        gaps[b] = tick - jnp.sum(found, axis=0, keepdims=True)
        return 0

    lax.fori_loop(0, n, gap_of, 0, unroll=2)

    for k in range(tiles):
        half = slice((k % per) * LANES, (k % per + 1) * LANES)
        where[k : k + 1, :] = pair[k // per : k // per + 1, half]

    def column(i, _):
        block, half = lax.div(i, per), lax.rem(i, per)
        node = node_row(block, half).astype(F32)
        columns[lanes_of(i, LANES), :] = jnp.broadcast_to(node, (LANES, LANES)).T
        return 0

    lax.fori_loop(0, tiles, column, 0, unroll=4)

    reply_in.wait_recv()

    for k in range(tiles):
        wide[k] = held[k // per, :, (k % per) * LANES : (k % per + 1) * LANES].astype(F32)

    def permute(block, _):
        for half in range(per):
            p = where[pl.ds(block * per + half, 1), :]
            tile = jnp.broadcast_to(lax.shift_right_logical(p, 7), (8, LANES))
            place = jnp.broadcast_to(lax.bitwise_and(p, LANES - 1), (8, LANES))
            parts = [jnp.zeros((8, LANES), F32) for _ in range(wp // 8)]
            for k in range(tiles):
                hit = tile == k
                for r in range(wp // 8):
                    got = jnp.take_along_axis(wide[k, r * 8 : (r + 1) * 8, :], place, axis=1)
                    parts[r] = jnp.where(hit, got, parts[r])
            whole = jnp.concatenate(parts, axis=0).astype(B16)
            perm[block, :, half * LANES : (half + 1) * LANES] = whole
        return 0

    lax.fori_loop(0, n, permute, 0)

    spreads = [
        remote(
            perm.at[others[k]],
            part_all.at[col, row],
            spread_s.at[0],
            spread_r.at[k],
            "rows",
            others[k],
        )
        for k in range(1, n)
    ]
    for copy in spreads:
        copy.start()

    def spread_in(k):
        return remote(
            perm.at[others[k]],
            part_all.at[col, sources[k]],
            spread_s.at[0],
            spread_r.at[k],
            "rows",
            others[k],
        )

    begin(0)
    part_all[col, row] = perm[row]

    def same_of(i, _):
        block, half = lax.div(i, per), lax.rem(i, per)
        same = columns[...] == node_row(block, half).astype(F32)
        equal[:, lanes_of(i, LANES)] = jnp.where(same, 1.0, 0.0).astype(B16)
        return 0

    for k in range(n):
        lax.fori_loop(k * per, (k + 1) * per, same_of, 0)
        if (k + 1) % (n // SELF_PARTS) == 0:
            forward_self(k // (n // SELF_PARTS))
    for k in range(1, n):
        spread_in(k).wait_recv()
        begin(k)

    few = pl.ds(0, c - 1)
    w_in = remote(w_src.at[few], w.at[few], w_s.at[0], w_r.at[0], "cols", mate(col, 1, c))
    w_in.wait_recv()
    w_self, w_part, w_time_all, w_hid_all = (
        w[:, k].reshape(c * wp, LANES)[:, 0:g3] for k in range(4)
    )
    to_row = iota((g3, g3), 0)
    to_gate = jnp.zeros((g3, g3), I32)
    for k in range(1, 3):
        to_gate = to_gate + jnp.where(to_row >= k * wp, 1, 0)
    hit = iota((g3, g3), 1) == 3 * (to_row - to_gate * wp) + to_gate
    bias_x, bias_h = spread_row(bias_in, hit), spread_row(bias_hid, hit)
    square = (freq.shape[1],) * 2
    diagonal = iota(square, 0) == iota(square, 1)
    rate, shift_by = spread_row(freq, diagonal), spread_row(phase, diagonal)
    acc[...] = jnp.zeros(acc.shape, F32)
    number[...] = jnp.zeros(number.shape, F32)

    def time_part(b, _):
        encoded = jnp.cos(gaps[b] * rate + shift_by).astype(B16)
        timed[:, lanes_of(b, cap)] = over_in(w_time_all, encoded)
        return 0

    early = n // 2 + 1
    lax.fori_loop(0, early, time_part, 0)
    for k in range(early, n):
        forward(k - early)
        lax.fori_loop(k, k + 1, time_part, 0)

    for k in range(SELF_PARTS):
        finish_self(k)

    def self_part(b, _):
        lanes = lanes_of(b, cap)
        xs = self_all[:, b].reshape(c * wp, cap)
        gx = over_in(w_self, xs) + bias_x
        gh = over_in(w_hid_all, xs) + bias_h
        pre[0 : 2 * wp, lanes] = gx[0 : 2 * wp] + gh[0 : 2 * wp]
        pre[2 * wp : 3 * wp, lanes] = gx[2 * wp :]
        pre[3 * wp :, lanes] = gh[2 * wp :]
        return 0

    lax.fori_loop(0, n, self_part, 0, unroll=4)

    def add_block(k):
        b = sources[k]
        xp = part_all[:, b].reshape(c * wp, cap)
        gi = over_in(w_part, xp) + timed[:, lanes_of(b, cap)]
        big = gi.astype(B16)
        both = jnp.concatenate(
            [big, (gi - big.astype(F32)).astype(B16), jnp.ones((16, cap), B16)], axis=0
        )
        mine = pl.ds(pl.multiple_of(b * cap, cap), cap)

        def into(i, _):
            lanes = lanes_of(i, cap)
            sums = jnp.dot(both, equal[mine, lanes], preferred_element_type=F32)
            acc[:, lanes] += sums[0:g3] + sums[g3 : 2 * g3]
            number[:, lanes] += sums[2 * g3 : 2 * g3 + 8]
            return 0

        lax.fori_loop(0, n, into, 0, unroll=8)

    sent = n - early
    for k in range(n):
        ahead = min(k + sent, n)
        if k + sent < n:
            forward(ahead)
        finish(k)
        add_block(k)

    def gates(b, _):
        lanes = lanes_of(b, cap)
        mean = acc[:, lanes] * (1.0 / number[0:1, lanes])
        rz = jax.nn.sigmoid(mean[0 : 2 * wp] + pre[0 : 2 * wp, lanes])
        reset, keep = rz[0:wp], rz[wp:]
        cand = jnp.tanh(mean[2 * wp :] + pre[2 * wp : 3 * wp, lanes] + reset * pre[3 * wp :, lanes])
        fresh[:, lanes] = (1.0 - keep) * cand + keep * own[:, lanes]
        return 0

    lax.fori_loop(0, n, gates, 0)

    remote(
        meta_src.at[rest], meta.at[rest], meta_s.at[0], meta_r.at[0], "rows", others[1]
    ).wait_send()
    remote(perm.at[rest], perm.at[rest], spread_s.at[0], spread_r.at[0], "rows", others[1]).wait_send()
    w_in.wait_send()
    reply_in.wait_send()
    drain_self()
    drain()


def scatter_kernel(ids, meta, fresh, _, out, rows, flat, turned, group_at, out_sem):
    n, per = ids.shape[0], ids.shape[1] // 2
    wp, node_rows = out.shape
    groups = LANES // wp
    rows_n = node_rows // groups
    tiles = n * per
    step = rows_n // PIECES

    def tile(i, _):
        value = fresh[:, lanes_of(i, LANES)]
        turned[lanes_of(i, LANES), :] = jnp.concatenate([value] * groups, axis=0).T
        b, half = lax.div(i, per), lax.rem(i, per)
        group = lax.shift_right_logical(meta[b, pl.ds(per + half, 1), :], SHIFT).astype(F32)
        group_at[lanes_of(i, LANES), :] = jnp.broadcast_to(group, (LANES, LANES)).T
        return 0

    lax.fori_loop(0, tiles, tile, 0, unroll=4)
    group_of = lax.div(iota((1, LANES), 1), wp).astype(F32)

    def slots(i, _):
        b, half = lax.div(i, per), lax.rem(i, per)
        for u in range(LANES):
            pltpu.store(
                rows.at[pl.ds(ids[b, half, u], 1), :],
                turned[pl.ds(i * LANES + u, 1), :],
                mask=group_of == group_at[pl.ds(i * LANES + u, 1), :],
            )
        return 0

    lax.fori_loop(0, tiles, slots, 0)
    per_piece = step // LANES

    def back(i, _):
        x = rows[lanes_of(i, LANES), :].T
        for k in range(groups):
            flat[:, lanes_of(k * (rows_n // LANES) + i, LANES)] = x[k * wp : (k + 1) * wp]
        return 0

    copies = []
    for i in range(PIECES):
        lax.fori_loop(i * per_piece, (i + 1) * per_piece, back, 0, unroll=8)
        for k in range(groups):
            part = pl.ds(k * rows_n + i * step, step)
            copies.append(pltpu.make_async_copy(flat.at[:, part], out.at[:, part], out_sem))
            copies[-1].start()
    pltpu.make_async_copy(flat, out, out_sem).wait()


def dma(*shape):
    return pltpu.SemaphoreType.DMA(shape)


def local(
    n,
    c,
    memory,
    last_tick,
    slot_node,
    slot_pair,
    slot_tick,
    block_count,
    time_freq,
    time_phase,
    w_pair,
    w_time,
    w_hidden,
    bias_input,
    bias_hidden,
):
    wp, node_rows = memory.shape
    cap = slot_node.shape[1]
    total = n * cap
    tiles = total // LANES
    per = cap // LANES
    g3 = 3 * wp
    groups = LANES // wp
    rows_n = node_rows // groups
    shape = jax.ShapeDtypeStruct
    vm = pltpu.VMEM
    kept = 4 * ((rows_n + 8) * LANES + wp * total + 2 * total)
    limit = VMEM_BYTES - kept - (1 << 20)
    small = (
        slot_node,
        slot_tick,
        block_count,
        slot_pair,
        last_tick.reshape(node_rows // LANES, LANES),
        w_pair,
        w_time,
        w_hidden,
        bias_input.reshape(1, g3),
        bias_hidden.reshape(1, g3),
        time_freq.reshape(1, -1),
        time_phase.reshape(1, -1),
    )
    meta, fresh, rows = pl.pallas_call(
        functools.partial(main_kernel, n, c),
        out_shape=(
            vm((n, 2 * per, LANES), I32),
            vm((wp, total), F32),
            vm((rows_n + 8, LANES), F32),
        ),
        in_specs=[HBM] * 13,
        out_specs=(VM, VM, VM),
        scratch_shapes=[
            *(vm(x.shape, x.dtype) for x in small),
            dma(len(small)),
            vm((wp, node_rows), F32),
            pltpu.SMEM((n, 2 * per, LANES), I32),
            vm((n, 2 * per, LANES), I32),
            vm((c, 4, wp, LANES), B16),
            vm((c, 4, wp, LANES), B16),
            vm((cap, LANES), F32),
            vm((wp, total), F32),
            vm((n, wp, cap), B16),
            vm((tiles, wp, LANES), F32),
            vm((tiles, LANES), I32),
            vm((n, wp, cap), B16),
            vm((c, n, wp, cap), B16),
            vm((c, n, wp, cap), B16),
            vm((n, 1, cap), F32),
            vm((total, LANES), F32),
            vm((total, total), B16),
            vm((8, total), F32),
            vm((g3, total), F32),
            vm((4 * wp, total), F32),
            vm((g3, total), F32),
            dma(PIECES),
            dma(n),
            dma(1),
            dma(n),
            dma(1),
            dma(1),
            dma(1),
            dma(1),
            dma(1),
            dma(n),
            dma(2 * c),
            dma(c, SELF_PARTS),
            dma(2 * c),
            dma(c, n),
        ],
        compiler_params=pltpu.CompilerParams(
            collective_id=1, has_side_effects=True, vmem_limit_bytes=limit
        ),
        name="exchange",
    )(*(pltpu.with_memory_space_constraint(x, pltpu.HBM) for x in (*small, memory)))
    return pl.pallas_call(
        scatter_kernel,
        out_shape=(shape((wp, node_rows), F32), vm((rows_n + 8, LANES), F32)),
        in_specs=[SM, VM, VM, VM],
        out_specs=(ANY, VM),
        scratch_shapes=[
            vm((wp, node_rows), F32),
            vm((total, LANES), F32),
            vm((total, LANES), F32),
            pltpu.SemaphoreType.DMA,
        ],
        input_output_aliases={3: 1},
        compiler_params=pltpu.CompilerParams(vmem_limit_bytes=4 * (wp * node_rows + 2 * total * LANES) + (6 << 20)),
        name="scatter",
    )(meta, meta, fresh, rows)[0]


def solution(mesh):
    placed = (
        P("cols", "rows"),
        P("rows"),
        P("rows", None),
        P("rows", None),
        P("rows", None),
        P("rows", None),
        P(),
        P(),
        P("cols", None, None),
        P("cols", None),
        P("cols", None),
        P("cols"),
        P("cols"),
    )
    return jax.shard_map(
        functools.partial(local, mesh.shape["rows"], mesh.shape["cols"]),
        mesh=mesh,
        in_specs=placed,
        out_specs=P("cols", "rows"),
        check_vma=False,
    )
```

```python
import functools
import math

import jax
import jax.numpy as jnp
from jax import lax
from jax.experimental import pallas as pl
from jax.experimental.pallas import tpu as pltpu
from jax.sharding import PartitionSpec as P

MESH = pl.DeviceIdType.MESH
LANES = 128
SHIFT = 16
VM = pl.BlockSpec(memory_space=pltpu.VMEM)
SM = pl.BlockSpec(memory_space=pltpu.SMEM)
ANY = pl.BlockSpec(memory_space=pl.ANY)
HBM = pl.BlockSpec(memory_space=pltpu.HBM)
PIECES = 4
VMEM_BYTES = 67_043_328
SELF_PARTS = 4
F32, I32, B16 = jnp.float32, jnp.int32, jnp.bfloat16


def mate(me, k, n, back=False):
    if n & (n - 1):
        return lax.rem(me + (n - k if back else k), n)
    out = me
    for i in range(n.bit_length() - 1):
        if k >> i & 1:
            out = out + (1 << i) * (1 - 2 * lax.rem(lax.div(me, 1 << i), 2))
    return out


def remote(src, dst, send, recv, axis, peer):
    return pltpu.make_async_remote_copy(
        src_ref=src,
        dst_ref=dst,
        send_sem=send,
        recv_sem=recv,
        device_id={axis: peer},
        device_id_type=MESH,
    )


def ladder(c, buffer, first, places, parts, sends, recvs):
    col = lax.axis_index("cols")
    ways = (True, False)
    n = len(places)
    each = n // parts

    def towards(steps, right):
        return col + steps if right else col - steps

    def has(d, right):
        return towards(-d, right) >= 0 if right else towards(-d, right) < c

    def fits(d, right):
        return towards(d, right) < c if right else towards(d, right) >= 0

    def send_sem(d, right):
        return sends.at[2 * d + right - 2]

    def slot(source, target):
        return lax.rem(source - target + c, c) - 1

    def hop(d, k, right, stride):
        source = towards(stride - d, right)
        ref = buffer.at[source, places[k]]
        return remote(
            first(k) if d == stride else ref,
            ref,
            send_sem(d, right),
            recvs.at[slot(source, towards(stride, right)), k // each],
            "cols",
            towards(stride, right),
        )

    def landed(d, part, right):
        source = towards(-d, right)
        peer = jnp.minimum(col + 1, c - 1) if right else jnp.maximum(col - 1, 0)
        ref = buffer.at[source, pl.ds(0, each)]
        return remote(ref, ref, send_sem(d, right), recvs.at[slot(source, col), part], "cols", peer)

    def when(*tests):
        return pl.when(functools.reduce(jnp.logical_and, tests))

    def begin(k):
        for d in (2, 1):
            for right in ways:
                if d < c:

                    @when(fits(d, right))
                    def _(d=d, right=right):
                        hop(d, k, right, d).start()

    def forward(part):
        for d in range(2, c - 1):
            for right in ways:

                @when(has(d, right), fits(1, right))
                def _(d=d, right=right):
                    landed(d, part, right).wait_recv()
                    for k in range(part * each, (part + 1) * each):
                        hop(d + 1, k, right, 1).start()

    def finish(part):
        for d in range(1, c):
            for right in ways:
                tests = [has(d, right)]
                if d > 1:
                    tests.append(jnp.logical_not(fits(1, right)))

                @when(*tests)
                def _(d=d, right=right):
                    landed(d, part, right).wait_recv()

    def drain():
        for right in ways:
            peer = jnp.minimum(col + 1, c - 1) if right else jnp.maximum(col - 1, 0)
            for d in range(1, c):
                if d < 3:
                    tests = [fits(d, right)]
                else:
                    tests = [has(d - 1, right), fits(1, right)]

                @when(*tests)
                def _(d=d, right=right, peer=peer):
                    ref = buffer.at[0]
                    remote(ref, ref, send_sem(d, right), recvs.at[0, 0], "cols", peer).wait_send()

    return begin, forward, finish, drain


def lanes_of(i, width):
    return pl.ds(pl.multiple_of(i * width, width), width)


def spread_row(ref, hit):
    return jnp.sum(jnp.where(hit, ref[...], 0.0), axis=1, keepdims=True)


def over_in(a, b):
    return lax.dot_general(a, b, (((0,), (0,)), ((), ())), preferred_element_type=F32)


SINE = [(-1) ** i * (2.0 * math.pi) ** (2 * i + 1) / math.factorial(2 * i + 1) for i in range(7)]


def cos_turns(x):
    big = 1.5 * 2.0**23
    x = 0.25 - jnp.abs(x - ((x + big) - big))
    square = x * x
    out = jnp.full_like(x, SINE[-1])
    for term in SINE[-2::-1]:
        out = out * square + term
    return out * x


def iota(shape, axis):
    return lax.broadcasted_iota(I32, shape, axis)


def main_kernel(n, c, *refs):
    given, memory, refs = refs[0:12], refs[12], refs[13:]
    outs, refs = refs[0:4], refs[4:]
    taken, in_sem, refs = refs[0:12], refs[12], refs[13:]
    fetches = [
        pltpu.make_async_copy(a, b, in_sem.at[i]) for i, (a, b) in enumerate(zip(given, taken))
    ]
    main_body(n, c, fetches, *taken, memory, *outs, *refs)


def main_body(
    n,
    c,
    fetches,
    nodes,
    ticks,
    counts,
    pair,
    last,
    w_pair,
    w_time,
    w_hid,
    bias_in,
    bias_hid,
    freq,
    phase,
    memory,
    meta,
    fresh,
    rows,
    columns,
    flat,
    ids,
    meta_src,
    w_src,
    w,
    picked_0,
    picked_1,
    own,
    held,
    wide,
    where,
    perm,
    self_all,
    part_all,
    gaps,
    equal,
    number,
    timed,
    pre,
    acc,
    load_sem,
    id_sem,
    meta_s,
    meta_r,
    w_s,
    w_r,
    reply_s,
    reply_r,
    spread_s,
    spread_r,
    *hops,
):
    row, col = lax.axis_index("rows"), lax.axis_index("cols")
    picked = (picked_0, picked_1)
    cap = nodes.shape[1]
    wp, node_rows = memory.shape
    groups = LANES // wp
    rows_n = node_rows // groups
    g3 = 3 * wp
    per = cap // LANES
    tiles = n * per
    width = c * g3

    def group_row(b, half):
        return lax.shift_right_logical(meta[b, pl.ds(per + half, 1), :], SHIFT)

    def node_row(b, half):
        return meta[b, pl.ds(half, 1), :] + group_row(b, half) * rows_n

    def wide_row(row_of, b):
        return jnp.concatenate([row_of(b, half) for half in range(per)], axis=1)

    barrier = pltpu.get_barrier_semaphore()
    for axis, size, me in (("rows", n, row), ("cols", c, col)):
        for k in range(1, size):
            pl.semaphore_signal(
                barrier, inc=1, device_id={axis: mate(me, k, size)}, device_id_type=MESH
            )

    for copy in fetches:
        copy.start()
    step = rows_n // PIECES
    loads = []
    for i in range(PIECES):
        for k in range(groups):
            part = pl.ds(k * rows_n + i * step, step)
            loads.append(pltpu.make_async_copy(memory.at[:, part], flat.at[:, part], load_sem.at[i]))
    for copy in loads:
        copy.start()

    lane = iota((1, cap), 1)
    for copy in fetches[0:3]:
        copy.wait()
    for b in range(n):
        mine = nodes[b : b + 1, :] - b * node_rows
        group = jnp.zeros((1, cap), I32)
        for k in range(1, groups):
            group = group + jnp.where(mine >= k * rows_n, 1, 0)
        live = lane < counts[0:1, b : b + 1]
        place = jnp.where(live, mine - group * rows_n, rows_n)
        rest_of = ticks[b : b + 1, :] + jnp.where(live, group, groups) * (1 << SHIFT)
        for half in range(per):
            lanes = slice(half * LANES, (half + 1) * LANES)
            meta_src[b, half : half + 1, :] = place[:, lanes]
            meta_src[b, per + half : per + half + 1, :] = rest_of[:, lanes]

    pl.semaphore_wait(barrier, n + c - 2)
    metas = [
        remote(
            meta_src.at[mate(row, k, n)],
            meta.at[row],
            meta_s.at[0],
            meta_r.at[k],
            "rows",
            mate(row, k, n),
        )
        for k in range(1, n)
    ]
    for copy in reversed(metas):
        copy.start()
    meta[row] = meta_src[row]

    sources = [mate(row, k, n, True) for k in range(n)]
    others = [mate(row, k, n) for k in range(n)]
    order = [0, 1, 2, *range(n - 1, 2, -1)]
    turns_of = [sources[k] for k in order]
    id_copies = [
        pltpu.make_async_copy(meta.at[b], ids.at[b], id_sem.at[i % 3])
        for i, b in enumerate(turns_of)
    ]

    def arrive(i):
        k = order[i]
        if k:
            remote(
                meta_src.at[others[k]],
                meta.at[sources[k]],
                meta_s.at[0],
                meta_r.at[k],
                "rows",
                others[k],
            ).wait_recv()
        id_copies[i].start()

    arrive(0)
    rows[rows_n:, :] = jnp.zeros((8, LANES), F32)
    per_piece = step // LANES

    def turn(i, _):
        block = [flat[:, lanes_of(k * (rows_n // LANES) + i, LANES)] for k in range(groups)]
        rows[lanes_of(i, LANES), :] = jnp.concatenate(block, 0).T
        return 0

    for i in range(PIECES):
        if i == 1:
            for copy in fetches[3:]:
                copy.wait()
            q = iota((1, LANES), 1)
            gate = jnp.zeros((1, LANES), I32)
            for k in range(1, 4):
                gate = gate + jnp.where(q >= k * wp, 1, 0)
            target = jnp.where(q < g3, 3 * (q - gate * wp) + gate, -width)
            stacked = jnp.concatenate([w_pair[:, 0, :], w_pair[:, 1, :], w_time[...], w_hid[...]], axis=0)
            from_col = iota((width, LANES), 0)
            for p in range(c):
                pick = jnp.where(from_col == target + p * g3, 1.0, 0.0).astype(B16)
                block = jnp.dot(stacked, pick, preferred_element_type=F32)
                kinds = [block[k * wp : (k + 1) * wp, 0:g3] for k in range(4)]
                w_src[p] = jnp.concatenate(kinds, axis=1).astype(B16)
            sends = [
                remote(
                    w_src.at[mate(col, k, c)], w.at[col], w_s.at[0], w_r.at[0], "cols", mate(col, k, c)
                )
                for k in range(1, c)
            ]
            for copy in sends:
                copy.start()
            w[col] = w_src[col]

        all_groups = pl.ds(0, groups * step)
        pltpu.make_async_copy(
            memory.at[:, all_groups], flat.at[:, all_groups], load_sem.at[i]
        ).wait()
        lax.fori_loop(i * per_piece, (i + 1) * per_piece, turn, 0, unroll=16)

    def reply(k):
        b = sources[k]
        return remote(
            self_all.at[col, b], held.at[row], reply_s.at[0], reply_r.at[0], "rows", b
        )

    rest = pl.ds(0, n - 1)
    reply_in = remote(
        self_all.at[col, rest], held.at[rest], reply_s.at[0], reply_r.at[0], "rows", others[1]
    )

    begin_self, forward_self, finish_self, drain_self = ladder(
        c, self_all, lambda i: self_all.at[col, turns_of[i]], turns_of, SELF_PARTS, *hops[0:2]
    )
    begin, forward, finish, drain = ladder(
        c,
        part_all,
        lambda k: part_all.at[col, sources[k]] if k else perm.at[row],
        sources,
        n,
        *hops[2:4],
    )

    def slots(i):
        b = turns_of[i]
        for half in range(per):
            for u in range(LANES):
                r = ids[b, half, u]
                picked[i % 2][half * LANES + u : half * LANES + u + 1, :] = rows[pl.ds(r, 1), :]

    def turn_back(i):
        b = turns_of[i]
        for half in range(per):
            lanes = slice(half * LANES, (half + 1) * LANES)
            group = group_row(b, half)
            turned = picked[i % 2][lanes, :].T
            mine = turned[0:wp]
            for g in range(1, groups):
                mine = jnp.where(group == g, turned[g * wp : (g + 1) * wp], mine)
            own[:, lanes_of(b * per + half, LANES)] = mine
            self_all[col, b, :, lanes] = mine.astype(B16)

    def send_own(i):
        if order[i]:
            reply(order[i]).start()
        else:
            held[row] = self_all[col, row]
        begin_self(i)

    arrive(1)
    for i in range(n):
        if i + 2 < n:
            arrive(i + 2)
        id_copies[i].wait()
        slots(i)
        if i:
            turn_back(i - 1)
            send_own(i - 1)
    turn_back(n - 1)
    send_own(n - 1)

    for k in range(tiles):
        half = slice((k % per) * LANES, (k % per + 1) * LANES)
        where[k : k + 1, :] = pair[k // per : k // per + 1, half]

    def column(i, _):
        block, half = lax.div(i, per), lax.rem(i, per)
        node = node_row(block, half).astype(F32)
        columns[lanes_of(i, LANES), :] = jnp.broadcast_to(node, (LANES, LANES)).T
        return 0

    lax.fori_loop(0, tiles, column, 0, unroll=4)

    forward_self(0)
    reply_in.wait_recv()

    for k in range(tiles):
        wide[k] = held[k // per, :, (k % per) * LANES : (k % per + 1) * LANES].astype(F32)

    def permute(block):
        for half in range(per):
            p = where[pl.ds(block * per + half, 1), :]
            tile = jnp.broadcast_to(lax.shift_right_logical(p, 7), (8, LANES))
            place = jnp.broadcast_to(lax.bitwise_and(p, LANES - 1), (8, LANES))
            parts = [jnp.zeros((8, LANES), F32) for _ in range(wp // 8)]
            for k in range(tiles):
                hit = tile == k
                for r in range(wp // 8):
                    got = jnp.take_along_axis(wide[k, r * 8 : (r + 1) * 8, :], place, axis=1)
                    parts[r] = jnp.where(hit, got, parts[r])
            whole = jnp.concatenate(parts, axis=0).astype(B16)
            perm[block, :, half * LANES : (half + 1) * LANES] = whole

    def spread_out(k):
        return remote(
            perm.at[others[k]],
            part_all.at[col, row],
            spread_s.at[0],
            spread_r.at[k],
            "rows",
            others[k],
        )

    permute(row)
    begin(0)
    part_all[col, row] = perm[row]
    for k in range(n - 1, 0, -1):
        permute(others[k])
        spread_out(k).start()

    def spread_in(k):
        return remote(
            perm.at[others[k]],
            part_all.at[col, sources[k]],
            spread_s.at[0],
            spread_r.at[k],
            "rows",
            others[k],
        )


    def same_of(i, _):
        block, half = lax.div(i, per), lax.rem(i, per)
        same = columns[...] == node_row(block, half).astype(F32)
        equal[:, lanes_of(i, LANES)] = jnp.where(same, 1.0, 0.0).astype(B16)
        return 0

    def pass_on(k):
        spread_in(k).wait_recv()
        begin(k)

    first_in = n // 4
    for k in range(n):
        lax.fori_loop(k * per, (k + 1) * per, same_of, 0)
        if k == first_in - 1:
            forward_self(1)
        if k >= first_in:
            pass_on(k - first_in + 1)
    forward_self(2)
    for k in range(n - first_in + 1, n):
        pass_on(k)

    hi_rows = node_rows // LANES
    old = last[...]
    table = jnp.concatenate(
        [lax.shift_right_logical(old, 8).astype(F32), lax.bitwise_and(old, 255).astype(F32)], axis=1
    ).astype(B16)
    hi_iota = iota((hi_rows, cap), 0)
    lo_iota = iota((LANES, cap), 0)

    def gap_of(b, _):
        node = wide_row(node_row, b)
        pick = jnp.where(hi_iota == lax.shift_right_logical(node, 7), 1.0, 0.0).astype(B16)
        found = over_in(table, pick)
        found = found[0:LANES] * 256.0 + found[LANES:]
        found = jnp.where(lo_iota == lax.bitwise_and(node, LANES - 1), found, 0.0)
        tick = wide_row(lambda b, half: meta[b, pl.ds(per + half, 1), :], b)
        tick = lax.bitwise_and(tick, (1 << SHIFT) - 1).astype(F32)
        gaps[b] = tick - jnp.sum(found, axis=0, keepdims=True)
        return 0

    lax.fori_loop(0, n, gap_of, 0, unroll=2)

    forward_self(3)
    few = pl.ds(0, c - 1)
    w_in = remote(w_src.at[few], w.at[few], w_s.at[0], w_r.at[0], "cols", mate(col, 1, c))
    w_in.wait_recv()
    w_self, w_part, w_time_all, w_hid_all = (
        w[...].reshape(c * wp, 4 * g3)[:, k * g3 : (k + 1) * g3] for k in range(4)
    )
    to_row = iota((g3, g3), 0)
    to_gate = jnp.zeros((g3, g3), I32)
    for k in range(1, 3):
        to_gate = to_gate + jnp.where(to_row >= k * wp, 1, 0)
    hit = iota((g3, g3), 1) == 3 * (to_row - to_gate * wp) + to_gate
    bias_x, bias_h = spread_row(bias_in, hit), spread_row(bias_hid, hit)
    square = (freq.shape[1],) * 2
    diagonal = iota(square, 0) == iota(square, 1)
    turns = 1.0 / (2.0 * math.pi)
    rate = spread_row(freq, diagonal) * turns
    shift_by = spread_row(phase, diagonal) * turns
    acc[...] = jnp.zeros(acc.shape, F32)
    number[...] = jnp.zeros(number.shape, F32)

    def time_part(b, _):
        encoded = cos_turns(gaps[b] * rate + shift_by).astype(B16)
        timed[:, lanes_of(b, cap)] = over_in(w_time_all, encoded)
        return 0

    lax.fori_loop(0, n, time_part, 0, unroll=2)

    for k in range(SELF_PARTS):
        finish_self(k)

    def self_part(b, _):
        lanes = lanes_of(b, cap)
        xs = self_all[:, b].reshape(c * wp, cap)
        gx = over_in(w_self, xs) + bias_x
        gh = over_in(w_hid_all, xs) + bias_h
        pre[0 : 2 * wp, lanes] = gx[0 : 2 * wp] + gh[0 : 2 * wp]
        pre[2 * wp : 3 * wp, lanes] = gx[2 * wp :]
        pre[3 * wp :, lanes] = gh[2 * wp :]
        return 0

    lax.fori_loop(0, n, self_part, 0, unroll=4)

    def add_block(k):
        b = sources[k]
        xp = part_all[:, b].reshape(c * wp, cap)
        gi = over_in(w_part, xp) + timed[:, lanes_of(b, cap)]
        big = gi.astype(B16)
        both = jnp.concatenate(
            [big, (gi - big.astype(F32)).astype(B16), jnp.ones((16, cap), B16)], axis=0
        )
        mine = pl.ds(pl.multiple_of(b * cap, cap), cap)

        def into(i, _):
            lanes = lanes_of(i, cap)
            sums = jnp.dot(both, equal[mine, lanes], preferred_element_type=F32)
            acc[:, lanes] += sums[0:g3] + sums[g3 : 2 * g3]
            number[:, lanes] += sums[2 * g3 : 2 * g3 + 8]
            return 0

        lax.fori_loop(0, n, into, 0, unroll=8)

    lag = 2
    for k in range(n + lag):
        if k < n:
            forward(k)
        if k >= lag:
            finish(k - lag)
            add_block(k - lag)

    def gates(b, _):
        lanes = lanes_of(b, cap)
        mean = acc[:, lanes] * (1.0 / number[0:1, lanes])
        rz = jax.nn.sigmoid(mean[0 : 2 * wp] + pre[0 : 2 * wp, lanes])
        reset, keep = rz[0:wp], rz[wp:]
        cand = jnp.tanh(mean[2 * wp :] + pre[2 * wp : 3 * wp, lanes] + reset * pre[3 * wp :, lanes])
        fresh[:, lanes] = (1.0 - keep) * cand + keep * own[:, lanes]
        return 0

    lax.fori_loop(0, n, gates, 0)

    remote(
        meta_src.at[rest], meta.at[rest], meta_s.at[0], meta_r.at[0], "rows", others[1]
    ).wait_send()
    remote(perm.at[rest], perm.at[rest], spread_s.at[0], spread_r.at[0], "rows", others[1]).wait_send()
    w_in.wait_send()
    reply_in.wait_send()
    drain_self()
    drain()


def scatter_kernel(meta, fresh, columns, _, out, rows, flat, ids, turned, id_sem, out_sem):
    n, per = meta.shape[0], meta.shape[1] // 2
    wp, node_rows = out.shape
    groups = LANES // wp
    rows_n = node_rows // groups
    tiles = n * per
    step = rows_n // (2 * PIECES)
    copy = pltpu.make_async_copy(meta, ids, id_sem)
    copy.start()

    start = lax.div(iota((1, LANES), 1), wp).astype(F32) * rows_n
    end = start + rows_n

    def turn(i):
        if i < tiles:
            lanes = slice(i * LANES, (i + 1) * LANES)
            turned[lanes, :] = jnp.concatenate([fresh[:, lanes]] * groups, axis=0).T

    ahead = 4
    for i in range(ahead):
        turn(i)
    copy.wait()
    for i in range(tiles):
        turn(i + ahead)
        b, half = i // per, i % per
        for u in range(i * LANES, (i + 1) * LANES):
            node = columns[u : u + 1, :]
            pltpu.store(
                rows.at[pl.ds(ids[b, half, u % LANES], 1), :],
                turned[u : u + 1, :],
                mask=jnp.logical_and(node >= start, node < end),
            )

    per_piece = step // LANES

    def back(i, _):
        x = rows[lanes_of(i, LANES), :].T
        for k in range(groups):
            flat[:, lanes_of(k * (rows_n // LANES) + i, LANES)] = x[k * wp : (k + 1) * wp]
        return 0

    copies = []
    for i in range(2 * PIECES):
        lax.fori_loop(i * per_piece, (i + 1) * per_piece, back, 0, unroll=8)
        for k in range(groups):
            part = pl.ds(k * rows_n + i * step, step)
            copies.append(pltpu.make_async_copy(flat.at[:, part], out.at[:, part], out_sem))
            copies[-1].start()
    pltpu.make_async_copy(flat, out, out_sem).wait()


def dma(*shape):
    return pltpu.SemaphoreType.DMA(shape)


def local(
    n,
    c,
    memory,
    last_tick,
    slot_node,
    slot_pair,
    slot_tick,
    block_count,
    time_freq,
    time_phase,
    w_pair,
    w_time,
    w_hidden,
    bias_input,
    bias_hidden,
):
    wp, node_rows = memory.shape
    cap = slot_node.shape[1]
    total = n * cap
    tiles = total // LANES
    per = cap // LANES
    g3 = 3 * wp
    groups = LANES // wp
    rows_n = node_rows // groups
    shape = jax.ShapeDtypeStruct
    vm = pltpu.VMEM
    kept = 4 * ((rows_n + 8) * LANES + wp * total + 2 * total + total * LANES)
    limit = VMEM_BYTES - kept - (1 << 20)
    small = (
        slot_node,
        slot_tick,
        block_count,
        slot_pair,
        last_tick.reshape(node_rows // LANES, LANES),
        w_pair,
        w_time,
        w_hidden,
        bias_input.reshape(1, g3),
        bias_hidden.reshape(1, g3),
        time_freq.reshape(1, -1),
        time_phase.reshape(1, -1),
    )
    meta, fresh, rows, columns = pl.pallas_call(
        functools.partial(main_kernel, n, c),
        out_shape=(
            vm((n, 2 * per, LANES), I32),
            vm((wp, total), F32),
            vm((rows_n + 8, LANES), F32),
            vm((total, LANES), F32),
        ),
        in_specs=[HBM] * 13,
        out_specs=(VM, VM, VM, VM),
        scratch_shapes=[
            *(vm(x.shape, x.dtype) for x in small),
            dma(len(small)),
            vm((wp, node_rows), F32),
            pltpu.SMEM((n, 2 * per, LANES), I32),
            vm((n, 2 * per, LANES), I32),
            vm((c, wp, 4 * g3), B16),
            vm((c, wp, 4 * g3), B16),
            vm((cap, LANES), F32),
            vm((cap, LANES), F32),
            vm((wp, total), F32),
            vm((n, wp, cap), B16),
            vm((tiles, wp, LANES), F32),
            vm((tiles, LANES), I32),
            vm((n, wp, cap), B16),
            vm((c, n, wp, cap), B16),
            vm((c, n, wp, cap), B16),
            vm((n, 1, cap), F32),
            vm((total, total), B16),
            vm((8, total), F32),
            vm((g3, total), F32),
            vm((4 * wp, total), F32),
            vm((g3, total), F32),
            dma(PIECES),
            dma(3),
            dma(1),
            dma(n),
            dma(1),
            dma(1),
            dma(1),
            dma(1),
            dma(1),
            dma(n),
            dma(2 * c - 2),
            dma(c - 1, SELF_PARTS),
            dma(2 * c - 2),
            dma(c - 1, n),
        ],
        compiler_params=pltpu.CompilerParams(
            collective_id=1, has_side_effects=True, vmem_limit_bytes=limit
        ),
        name="exchange",
    )(*(pltpu.with_memory_space_constraint(x, pltpu.HBM) for x in (*small, memory)))
    return pl.pallas_call(
        scatter_kernel,
        out_shape=(shape((wp, node_rows), F32), vm((rows_n + 8, LANES), F32)),
        in_specs=[VM, VM, VM, VM],
        out_specs=(ANY, VM),
        scratch_shapes=[
            vm((wp, node_rows), F32),
            pltpu.SMEM((n, 2 * per, LANES), I32),
            vm((total, LANES), F32),
            pltpu.SemaphoreType.DMA,
            pltpu.SemaphoreType.DMA,
        ],
        input_output_aliases={3: 1},
        compiler_params=pltpu.CompilerParams(vmem_limit_bytes=4 * (wp * node_rows + total * LANES) + (6 << 20)),
        name="scatter",
    )(meta, fresh, columns, rows)[0]


def solution(mesh):
    placed = (
        P("cols", "rows"),
        P("rows"),
        P("rows", None),
        P("rows", None),
        P("rows", None),
        P("rows", None),
        P(),
        P(),
        P("cols", None, None),
        P("cols", None),
        P("cols", None),
        P("cols"),
        P("cols"),
    )
    return jax.shard_map(
        functools.partial(local, mesh.shape["rows"], mesh.shape["cols"]),
        mesh=mesh,
        in_specs=placed,
        out_specs=P("cols", "rows"),
        check_vma=False,
    )
```
